16 devices in a mesh: dep: 2 (over z), col: 2 (over y), row: 4 (over x, core).
Axes of the slice: x: 2, y: 2, z: 2, core: 2. Of those that a mesh axis runs over, the one named last changes fastest.
Arguments:
- a_mat: bfloat16 [5120, 5120], P('row', 'col')
- b_mat: bfloat16 [5120, 5120], P('row', 'col')
Outputs:
- output: float32 [5120, 5120], P('row', ('col', 'dep'))
All inputs are finite; a program needn't handle non-finite values.
Results may differ from the reference program's by a relative error of at most 0.001.
Values are sent between devices in bfloat16 or wider.
A program may use at most 1 GiB of HBM per device.

```python
import jax
import jax.numpy as jnp

N = 5120


def setup_inputs(seed: int = 0) -> dict:
    key = jax.random.key(seed)
    key_a, key_b = jax.random.split(key)
    a_mat = (jax.random.normal(key_a, (N, N), jnp.float32) * N ** -0.5).astype(jnp.bfloat16)
    b_mat = jax.random.normal(key_b, (N, N), jnp.float32).astype(jnp.bfloat16)
    return {"a_mat": a_mat, "b_mat": b_mat}


def reference(a_mat, b_mat):
    return jnp.dot(a_mat, b_mat, preferred_element_type=jnp.float32)
```

```python
import functools

import jax
import jax.numpy as jnp
from jax import lax
from jax.experimental import pallas as pl
from jax.experimental.pallas import tpu as pltpu
from jax.sharding import PartitionSpec as P

MESH = pl.DeviceIdType.MESH
STEPS = 10
SUBS = 5
CHUNK = 128
ROWS = 256
COLS = 256
TOTAL = STEPS * SUBS
AHEAD = 6
LAG_IN = 4
LAG = 8


def _kernel(a_ref, b_ref, c_ref, abuf, bbuf, ys, yr, zs, zr, xs, xr, ds, dr, bs, br, la, lb):
    z, y, r = lax.axis_index("dep"), lax.axis_index("col"), lax.axis_index("row")
    quarter = a_ref.shape[1] // 2
    across = lax.rem(r + 2, 4)
    peer = r + 1 - 2 * lax.rem(r, 2)
    peer_across = lax.rem(peer + 2, 4)
    to_y, to_z, to_x, to_d = {"col": 1 - y}, {"dep": 1 - z}, {"row": across}, {"row": peer}

    def lanes(q):
        return pl.ds(pl.multiple_of(q * CHUNK, CHUNK), CHUNK)

    def remote(src, dst, send, recv, to):
        return pltpu.make_async_remote_copy(
            src_ref=src, dst_ref=dst, send_sem=send, recv_sem=recv, device_id=to, device_id_type=MESH
        )

    def a_slot(t, s, q):
        return abuf.at[t, pl.ds(s * ROWS, ROWS), lanes(q)]

    def b_slot(t, s, q):
        return bbuf.at[t, lanes(q), pl.ds(s * COLS, COLS)]

    def y_copy(t, s, part=z, sem=None):
        sem = t * SUBS + s if sem is None else sem
        src = a_ref.at[pl.ds(s * ROWS, ROWS), pl.ds(pl.multiple_of(part * quarter + t * CHUNK, CHUNK), CHUNK)]
        return remote(src, a_slot(t, s, 2 * y + part), ys.at[sem], yr.at[sem], to_y)

    def y_in(t, s, part=z, sem=None):
        sem = t * SUBS + s if sem is None else sem
        slot = a_slot(t, s, 2 * (1 - y) + part)
        return remote(slot, slot, ys.at[sem], yr.at[sem], to_y)

    def z_copy(t, s):
        slot = a_slot(t, s, 2 * (1 - y) + z)
        return remote(slot, slot, zs.at[t * SUBS + s], zr.at[t * SUBS + s], to_z)

    def z_in(t, s):
        slot = a_slot(t, s, 2 * (1 - y) + 1 - z)
        return remote(slot, slot, zs.at[t * SUBS + s], zr.at[t * SUBS + s], to_z)

    def x_copy(t, s):
        src = b_ref.at[
            pl.ds(pl.multiple_of(t * CHUNK, CHUNK), CHUNK),
            pl.ds(pl.multiple_of(z * quarter + s * COLS, CHUNK), COLS),
        ]
        return remote(src, b_slot(t, s, r), xs.at[t * SUBS + s], xr.at[t * SUBS + s], to_x)

    def x_in(t, s):
        slot = b_slot(t, s, across)
        return remote(slot, slot, xs.at[t * SUBS + s], xr.at[t * SUBS + s], to_x)

    def d_copy(t, s):
        slot = b_slot(t, s, across)
        return remote(slot, slot, ds.at[t * SUBS + s], dr.at[t * SUBS + s], to_d)

    def d_in(t, s):
        slot = b_slot(t, s, peer_across)
        return remote(slot, slot, ds.at[t * SUBS + s], dr.at[t * SUBS + s], to_d)

    def b_rows(t):
        return b_ref.at[
            pl.ds(pl.multiple_of(t * CHUNK, CHUNK), CHUNK), pl.ds(pl.multiple_of(z * quarter, CHUNK), quarter)
        ]

    def peer_copy(t):
        return remote(b_rows(t), bbuf.at[t, lanes(r)], bs.at[t], br.at[t], to_d)

    def peer_in(t):
        slot = bbuf.at[t, lanes(peer)]
        return remote(slot, slot, bs.at[t], br.at[t], to_d)

    def b_load(t):
        return pltpu.make_async_copy(b_rows(t), bbuf.at[t, lanes(r)], lb.at[t])

    def a_load(t, part):
        src = a_ref.at[:, pl.ds(pl.multiple_of(part * quarter + t * CHUNK, CHUNK), CHUNK)]
        return pltpu.make_async_copy(src, abuf.at[t, :, lanes(2 * y + part)], la.at[2 * t + part])

    def step_of(n):
        return (n // SUBS, n % SUBS)

    def start_local(t):
        peer_copy(t).start()
        b_load(t).start()
        a_load(t, 0).start()
        a_load(t, 1).start()

    def wait_local(t):
        peer_copy(t).wait_send()
        peer_in(t).wait_recv()
        b_load(t).wait()
        a_load(t, 0).wait()
        a_load(t, 1).wait()

    def product(t, p):
        cols = pl.ds(p * COLS, COLS)
        c_ref[:, cols] += jnp.dot(abuf[t], bbuf[t, :, cols], preferred_element_type=jnp.float32)

    barrier = pltpu.get_barrier_semaphore()
    for to in (to_x, to_y, to_z, to_d):
        pl.semaphore_signal(barrier, inc=1, device_id=to, device_id_type=MESH)
    pl.semaphore_wait(barrier, 4)

    for n in range(AHEAD):
        y_copy(*step_of(n)).start()
        x_copy(*step_of(n)).start()
    start_local(0)
    start_local(1)
    c_ref[...] = jnp.zeros_like(c_ref)

    def arrive(t, s, last):
        y_in(t, s).wait_recv()
        if not (last and s == SUBS - 1):
            z_copy(t, s).start()
        x_in(t, s).wait_recv()
        d_copy(t, s).start()

    def settle(t, s):
        y_copy(t, s).wait_send()
        x_copy(t, s).wait_send()
        z_copy(t, s).wait_send()
        d_copy(t, s).wait_send()
        z_in(t, s).wait_recv()
        d_in(t, s).wait_recv()

    def body(t, carry):
        @pl.when(t + 2 < STEPS)
        def _():
            start_local(t + 2)

        for s in range(SUBS):
            arrive(t, s, False)

            dt, s2 = step_of(s + AHEAD)

            @pl.when(t + dt < STEPS)
            def _(dt=dt, s2=s2):
                y_copy(t + dt, s2).start()
                x_copy(t + dt, s2).start()

            dt, s2 = (s - LAG_IN) // SUBS, (s - LAG_IN) % SUBS

            @pl.when(t + dt >= 0)
            def _(dt=dt, s2=s2):
                settle(t + dt, s2)

            dt, s2 = (s - LAG) // SUBS, (s - LAG) % SUBS

            @pl.when(t + dt >= 0)
            def _(dt=dt, s2=s2):
                if s2 == 0:
                    wait_local(t + dt)
                product(t + dt, s2)

        return carry

    lax.fori_loop(0, STEPS - 1, body, 0)

    last = STEPS - 1
    done_in = last * SUBS - LAG_IN
    done_mul = last * SUBS - LAG
    extra = (last, SUBS - 1)
    y_copy(*extra, part=1 - z, sem=TOTAL).start()
    for s in range(SUBS):
        n = last * SUBS + s
        arrive(last, s, True)
        while done_in <= n - LAG_IN:
            settle(*step_of(done_in))
            done_in += 1
        while done_mul < done_in - SUBS + 1 and done_mul < last * SUBS:
            t, p = step_of(done_mul)
            if p == 0:
                wait_local(t)
            product(t, p)
            done_mul += 1
    while done_in < TOTAL:
        t, s = step_of(done_in)
        if done_in < TOTAL - 1:
            settle(t, s)
        else:
            y_copy(t, s).wait_send()
            x_copy(t, s).wait_send()
            d_copy(t, s).wait_send()
            d_in(t, s).wait_recv()
            y_copy(t, s, part=1 - z, sem=TOTAL).wait_send()
            y_in(t, s, part=1 - z, sem=TOTAL).wait_recv()
        done_in += 1
        while done_mul < done_in - SUBS + 1:
            t, p = step_of(done_mul)
            if p == 0:
                wait_local(t)
            product(t, p)
            done_mul += 1
    while done_mul < TOTAL:
        t, p = step_of(done_mul)
        if p == 0:
            wait_local(t)
        product(t, p)
        done_mul += 1


def solution(mesh):
    def local_product(a_blk, b_blk):
        rows, half = a_blk.shape
        piece = half // 2
        return pl.pallas_call(
            _kernel,
            out_shape=jax.ShapeDtypeStruct((rows, piece), jnp.float32),
            in_specs=[pl.BlockSpec(memory_space=pltpu.HBM)] * 2,
            out_specs=pl.BlockSpec(memory_space=pltpu.VMEM),
            scratch_shapes=[
                pltpu.VMEM((STEPS, rows, 4 * CHUNK), jnp.bfloat16),
                pltpu.VMEM((STEPS, 4 * CHUNK, piece), jnp.bfloat16),
                pltpu.SemaphoreType.DMA((TOTAL + 1,)),
                pltpu.SemaphoreType.DMA((TOTAL + 1,)),
                pltpu.SemaphoreType.DMA((TOTAL,)),
                pltpu.SemaphoreType.DMA((TOTAL,)),
                pltpu.SemaphoreType.DMA((TOTAL,)),
                pltpu.SemaphoreType.DMA((TOTAL,)),
                pltpu.SemaphoreType.DMA((TOTAL,)),
                pltpu.SemaphoreType.DMA((TOTAL,)),
                pltpu.SemaphoreType.DMA((STEPS,)),
                pltpu.SemaphoreType.DMA((STEPS,)),
                pltpu.SemaphoreType.DMA((2 * STEPS,)),
                pltpu.SemaphoreType.DMA((STEPS,)),
            ],
            compiler_params=pltpu.CompilerParams(collective_id=0, has_side_effects=True, vmem_limit_bytes=45 * 2**20),
            cost_estimate=pl.CostEstimate(flops=2 * rows * piece * 2 * half, bytes_accessed=40 * 2**20, transcendentals=0),
        )(a_blk, b_blk)

    return jax.shard_map(
        local_product,
        mesh=mesh,
        in_specs=(P("row", "col"), P("row", "col")),
        out_specs=P("row", ("col", "dep")),
        check_vma=False,
    )
```

```python
import jax
import jax.numpy as jnp
from jax import lax
from jax.experimental import pallas as pl
from jax.experimental.pallas import tpu as pltpu
from jax.sharding import PartitionSpec as P

MESH = pl.DeviceIdType.MESH
STEPS = 10
SUBS = 10
CHUNK = 128
PIECE = 128
COLS = 256
TOTAL = STEPS * SUBS
LAST = STEPS - 1
EXTRA = 3
AHEAD = 6
LAG = 6
RING = 2 * AHEAD
STEP_RING = 4
TAIL = (STEPS - 2) * SUBS
LIMIT = 42 * 2**20
LIMIT_FINISH = 20 * 2**20


def _exchange(a_ref, b_ref, c_ref, a_last, b_last, abuf, bbuf, yr, zr, xr, dr, sent, local):
    z, y, r = lax.axis_index("dep"), lax.axis_index("col"), lax.axis_index("row")
    quarter = a_ref.shape[1] // 2
    across = lax.rem(r + 2, 4)
    peer = r + 1 - 2 * lax.rem(r, 2)
    peer_across = lax.rem(peer + 2, 4)
    to_y, to_z, to_x, to_d = {"col": 1 - y}, {"dep": 1 - z}, {"row": across}, {"row": peer}

    def aligned(start, size):
        return pl.ds(pl.multiple_of(start, CHUNK), size)

    def lanes(q):
        return aligned(q * CHUNK, CHUNK)

    def remote(src, dst, send, recv, to):
        return pltpu.make_async_remote_copy(
            src_ref=src, dst_ref=dst, send_sem=send, recv_sem=recv, device_id=to, device_id_type=MESH
        )

    def is_last(t):
        return isinstance(t, int) and t == LAST

    def a_step(t):
        return a_last if is_last(t) else abuf.at[t]

    def b_step(t):
        return b_last if is_last(t) else bbuf.at[t]

    def a_slot(n, q):
        return a_step(n // SUBS).at[aligned((n % SUBS) * PIECE, PIECE), lanes(q)]

    def b_slot(n, q):
        return b_step(n // SUBS).at[lanes(q), aligned((n % SUBS) * PIECE, PIECE)]

    def take(some, sem):
        pltpu.make_async_copy(some, some, sem).wait()

    def step_sem(sems, t):
        return sems.at[STEP_RING if is_last(t) else lax.rem(t, STEP_RING)]

    def y_start(n):
        extra = isinstance(n, int) and n >= TOTAL
        part, send, recv = (1 - z, 4, RING) if extra else (z, 0, lax.rem(n, RING))
        n = n - EXTRA if extra else n
        src = a_ref.at[aligned((n % SUBS) * PIECE, PIECE), aligned(part * quarter + n // SUBS * CHUNK, CHUNK)]
        remote(src, a_slot(n, 2 * y + part), sent.at[send], yr.at[recv], to_y).start()

    def y_wait(n):
        take(a_slot(n, 2 * (1 - y) + z), yr.at[lax.rem(n, RING)])

    def z_start(n):
        slot = a_slot(n, 2 * (1 - y) + z)
        t = n // SUBS
        remote(slot, slot, sent.at[5 if is_last(t) else 1], step_sem(zr, t), to_z).start()

    def x_start(n):
        src = b_ref.at[aligned(n // SUBS * CHUNK, CHUNK), aligned(z * quarter + (n % SUBS) * PIECE, PIECE)]
        remote(src, b_slot(n, r), sent.at[2], xr.at[lax.rem(n, RING)], to_x).start()

    def x_wait(n):
        take(b_slot(n, across), xr.at[lax.rem(n, RING)])

    def d_start(n):
        slot = b_slot(n, across)
        remote(slot, slot, sent.at[3], step_sem(dr, n // SUBS), to_d).start()

    def settle(t):
        if is_last(t):
            take(a_last.at[pl.ds(0, (SUBS - EXTRA) * PIECE), lanes(2 * (1 - y) + 1 - z)], step_sem(zr, t))
            take(a_last.at[pl.ds(0, EXTRA * PIECE), lanes(2 * (1 - y) + 1 - z)], yr.at[RING])
        else:
            take(abuf.at[t, :, lanes(2 * (1 - y) + 1 - z)], step_sem(zr, t))
        take(b_step(t).at[lanes(peer_across)], step_sem(dr, t))

    def start_local():
        for t in range(STEPS):
            sems = 4 * (t // LAST)
            for part in range(2):
                src = a_ref.at[:, pl.ds(part * quarter + t * CHUNK, CHUNK)]
                pltpu.make_async_copy(src, a_step(t).at[:, lanes(2 * y + part)], local.at[sems]).start()
            src = b_ref.at[pl.ds(t * CHUNK, CHUNK), aligned(z * quarter, quarter)]
            dst = b_step(t).at[lanes(r)]
            pltpu.make_async_copy(src, dst, local.at[sems + 1]).start()
            remote(src, dst, local.at[sems + 2], local.at[sems + 3], to_d).start()

    def wait_local():
        take(abuf.at[:, :, pl.ds(0, 2 * CHUNK)], local.at[0])
        take(a_last.at[:, pl.ds(0, 2 * CHUNK)], local.at[4])
        for i, place in ((1, r), (2, r), (3, peer)):
            take(bbuf.at[:, lanes(place)], local.at[i])
            take(b_last.at[lanes(place)], local.at[4 + i])

    def product(t, p):
        cols = pl.ds(p * COLS, COLS)
        c_ref[:, cols] += jnp.dot(abuf[t], bbuf[t, :, cols], preferred_element_type=jnp.float32)

    barrier = pltpu.get_barrier_semaphore()
    for to in (to_x, to_y, to_z, to_d):
        pl.semaphore_signal(barrier, inc=1, device_id=to, device_id_type=MESH)
    pl.semaphore_wait(barrier, 4)

    for n in range(AHEAD):
        y_start(n)
        x_start(n)
    start_local()
    c_ref[...] = jnp.zeros_like(c_ref)

    def forward(n):
        known = isinstance(n, int)
        y_wait(n)
        if not known or n < TOTAL - EXTRA:
            z_start(n)
        if not known or n + AHEAD < TOTAL + EXTRA:
            y_start(n + AHEAD)
        x_wait(n)
        d_start(n)
        if not known or n + AHEAD < TOTAL:
            x_start(n + AHEAD)

    def body(t, carry):
        for s in range(SUBS):
            forward(t * SUBS + s)
            dt, i = (s - LAG) // SUBS - 1, (s - LAG) % SUBS
            if i % 2 == 0:

                @pl.when(t + dt >= 0)
                def _(dt=dt, i=i):
                    if i == 0:
                        pl.when(t + dt == 0)(wait_local)
                        settle(t + dt)
                    product(t + dt, i // 2)

        return carry

    lax.fori_loop(0, TAIL // SUBS, body, 0)

    work = [(t, p) for t in (STEPS - 4, STEPS - 3, STEPS - 2) for p in range(SUBS // 2)]
    begun = TAIL - (STEPS - 3) * SUBS - LAG
    work = work[(begun + 1) // 2 :]
    for n in range(TAIL, TOTAL):
        forward(n)
        t, p = work[0] if work else (LAST, 0)
        first = (t + 1) * SUBS + LAG
        if t < LAST and n >= first + (2 * p if t < LAST - 1 else p):
            if p == 0:
                settle(t)
            product(t, p)
            work.pop(0)
    for t, p in work:
        if p == 0:
            settle(t)
        product(t, p)
    settle(LAST)
    for i in (0, 2, 3):
        take(b_ref.at[:, pl.ds(0, quarter)], sent.at[i])
    take(abuf.at[:, :, pl.ds(0, CHUNK)], sent.at[1])
    take(a_last.at[pl.ds(0, EXTRA * PIECE), pl.ds(0, CHUNK)], sent.at[4])
    take(a_last.at[pl.ds(0, (SUBS - EXTRA) * PIECE), pl.ds(0, CHUNK)], sent.at[5])


def _finish(c_part, a_last, b_last, c_ref, done, sems):
    copies = []
    for i in range(SUBS):
        rows = pl.ds(i * PIECE, PIECE)
        done[rows] = c_part[rows] + jnp.dot(a_last[rows], b_last[...], preferred_element_type=jnp.float32)
        copies.append(pltpu.make_async_copy(done.at[rows], c_ref.at[rows], sems.at[i]))
        copies[-1].start()
    for copy in copies:
        copy.wait()


def solution(mesh):
    def local_product(a_blk, b_blk):
        rows, half = a_blk.shape
        piece = half // 2
        vmem = pl.BlockSpec(memory_space=pltpu.VMEM)
        hbm = pl.BlockSpec(memory_space=pltpu.HBM)
        parts = pl.pallas_call(
            _exchange,
            out_shape=[
                jax.ShapeDtypeStruct((rows, piece), jnp.float32),
                jax.ShapeDtypeStruct((rows, 4 * CHUNK), jnp.bfloat16),
                jax.ShapeDtypeStruct((4 * CHUNK, piece), jnp.bfloat16),
            ],
            in_specs=[hbm, hbm],
            out_specs=[vmem] * 3,
            scratch_shapes=[
                pltpu.VMEM((LAST, rows, 4 * CHUNK), jnp.bfloat16),
                pltpu.VMEM((LAST, 4 * CHUNK, piece), jnp.bfloat16),
                pltpu.SemaphoreType.DMA((RING + 1,)),
                pltpu.SemaphoreType.DMA((STEP_RING + 1,)),
                pltpu.SemaphoreType.DMA((RING,)),
                pltpu.SemaphoreType.DMA((STEP_RING + 1,)),
                pltpu.SemaphoreType.DMA((6,)),
                pltpu.SemaphoreType.DMA((8,)),
            ],
            compiler_params=pltpu.CompilerParams(collective_id=0, has_side_effects=True, vmem_limit_bytes=LIMIT),
        )(a_blk, b_blk)
        return pl.pallas_call(
            _finish,
            out_shape=jax.ShapeDtypeStruct((rows, piece), jnp.float32),
            in_specs=[vmem] * 3,
            out_specs=hbm,
            scratch_shapes=[pltpu.VMEM((rows, piece), jnp.float32), pltpu.SemaphoreType.DMA((SUBS,))],
            compiler_params=pltpu.CompilerParams(vmem_limit_bytes=LIMIT_FINISH),
        )(*parts)

    return jax.shard_map(
        local_product,
        mesh=mesh,
        in_specs=(P("row", "col"), P("row", "col")),
        out_specs=P("row", ("col", "dep")),
        check_vma=False,
    )
```

```python
import jax
import jax.numpy as jnp
from jax import lax
from jax.experimental import pallas as pl
from jax.experimental.pallas import tpu as pltpu
from jax.sharding import PartitionSpec as P

MESH = pl.DeviceIdType.MESH
STEPS = 10
SUBS = 10
CHUNK = 128
PIECE = 128
COLS = 256
TOTAL = STEPS * SUBS
LAST = STEPS - 1
EXTRA = 384
EARLY = 3
AHEAD = 7
WIDE = 5
B_AHEAD = 2
LAG = 6
RING = 2 * AHEAD
B_RING = 2 * B_AHEAD
B_SUBS = SUBS // WIDE
B_TOTAL = STEPS * B_SUBS
STEP_RING = 3
TAIL = (STEPS - 2) * SUBS
LIMIT = 42 * 2**20
LIMIT_FINISH = 20 * 2**20


def _exchange(a_ref, b_ref, c_ref, a_last, b_last, abuf, bbuf, yr, zr, xr, dr, sent, local, ready):
    z, y, r = lax.axis_index("dep"), lax.axis_index("col"), lax.axis_index("row")
    quarter = a_ref.shape[1] // 2
    across = lax.rem(r + 2, 4)
    peer = r + 1 - 2 * lax.rem(r, 2)
    peer_across = lax.rem(peer + 2, 4)
    to_y, to_z, to_x, to_d = {"col": 1 - y}, {"dep": 1 - z}, {"row": across}, {"row": peer}

    def aligned(start, size):
        return pl.ds(pl.multiple_of(start, CHUNK), size)

    def lanes(q):
        return aligned(q * CHUNK, CHUNK)

    def remote(src, dst, send, recv, to):
        return pltpu.make_async_remote_copy(
            src_ref=src, dst_ref=dst, send_sem=send, recv_sem=recv, device_id=to, device_id_type=MESH
        )

    def is_last(t):
        return isinstance(t, int) and t == LAST

    def a_step(t):
        return a_last if is_last(t) else abuf.at[t]

    def b_step(t):
        return b_last if is_last(t) else bbuf.at[t]

    def a_slot(n, q):
        return a_step(n // SUBS).at[aligned((n % SUBS) * PIECE, PIECE), lanes(q)]

    def b_slot(n, q):
        return b_step(n // B_SUBS).at[lanes(q), aligned((n % B_SUBS) * WIDE * PIECE, WIDE * PIECE)]

    def take(some, sem):
        pltpu.make_async_copy(some, some, sem).wait()

    def step_sem(sems, t):
        return sems.at[lax.rem(t, STEP_RING)]

    def y_start(n):
        if isinstance(n, int) and n == TOTAL:
            rows = pl.ds(SUBS * PIECE - EXTRA, EXTRA)
            src = a_ref.at[rows, aligned((1 - z) * quarter + LAST * CHUNK, CHUNK)]
            remote(src, a_last.at[rows, lanes(2 * y + 1 - z)], sent.at[0], yr.at[RING], to_y).start()
            return
        src = a_ref.at[aligned((n % SUBS) * PIECE, PIECE), aligned(z * quarter + n // SUBS * CHUNK, CHUNK)]
        remote(src, a_slot(n, 2 * y + z), sent.at[0], yr.at[lax.rem(n, RING)], to_y).start()

    def y_wait(n):
        take(a_slot(n, 2 * (1 - y) + z), yr.at[lax.rem(n, RING)])

    def z_start(n):
        slot, recv = a_slot(n, 2 * (1 - y) + z), step_sem(zr, n // SUBS)
        if is_last(n // SUBS):
            i = n % SUBS
            size = min(PIECE, SUBS * PIECE - EXTRA - i * PIECE)
            if size <= 0:
                return
            slot = a_last.at[pl.ds(i * PIECE, size), lanes(2 * (1 - y) + z)]
            recv = zr.at[STEP_RING] if i < EARLY else recv
        remote(slot, slot, sent.at[0], recv, to_z).start()

    def x_start(n):
        columns = aligned(z * quarter + (n % B_SUBS) * WIDE * PIECE, WIDE * PIECE)
        src = b_ref.at[aligned(n // B_SUBS * CHUNK, CHUNK), columns]
        remote(src, b_slot(n, r), sent.at[1], xr.at[lax.rem(n, B_RING)], to_x).start()

    def x_wait(n):
        take(b_slot(n, across), xr.at[lax.rem(n, B_RING)])

    def d_start(n):
        slot = b_slot(n, across)
        remote(slot, slot, sent.at[1], step_sem(dr, n // B_SUBS), to_d).start()

    def settle(t):
        take(abuf.at[t, :, lanes(2 * (1 - y) + 1 - z)], step_sem(zr, t))
        take(bbuf.at[t, lanes(peer_across)], step_sem(dr, t))

    def start_local():
        for t in range(STEPS):
            for part in range(2):
                src = a_ref.at[:, pl.ds(part * quarter + t * CHUNK, CHUNK)]
                pltpu.make_async_copy(src, a_step(t).at[:, lanes(2 * y + part)], local.at[0]).start()
            src = b_ref.at[pl.ds(t * CHUNK, CHUNK), aligned(z * quarter, quarter)]
            dst = b_step(t).at[lanes(r)]
            pltpu.make_async_copy(src, dst, local.at[1]).start()
            remote(src, dst, local.at[2], local.at[3], to_d).start()

    def wait_local():
        take(a_ref, local.at[0])
        for i in (1, 2, 3):
            take(b_ref.at[:, pl.ds(0, quarter)], local.at[i])

    def product(t, p):
        cols = pl.ds(p * COLS, COLS)
        c_ref[:, cols] += jnp.dot(abuf[t], bbuf[t, :, cols], preferred_element_type=jnp.float32)

    x = r // 2
    axes = ((x, to_x), (y, to_y), (z, to_z))
    barrier = pltpu.get_barrier_semaphore()
    for at, to in axes:

        @pl.when(at == 0)
        def _(to=to):
            pl.semaphore_signal(barrier, inc=1, device_id=to, device_id_type=MESH)

    pl.semaphore_signal(barrier, inc=1, device_id=to_d, device_id_type=MESH)
    pl.semaphore_wait(barrier, 1 + x + y + z)
    for i, (at, to) in enumerate(axes):

        @pl.when(at == 1)
        def _(i=i, to=to):
            pl.semaphore_signal(ready.at[i], inc=1, device_id=to, device_id_type=MESH)

    def begin(i):
        for n in range((B_AHEAD, AHEAD)[i]):
            (x_start, y_start)[i](n)

    pl.when(y == 1)(lambda: begin(1))
    pl.when(x == 1)(lambda: begin(0))
    start_local()
    for i in (1, 0):

        @pl.when(axes[i][0] == 0)
        def _(i=i):
            pl.semaphore_wait(ready.at[i], 1)
            begin(i)

    pl.when(z == 0)(lambda: pl.semaphore_wait(ready.at[2], 1))
    c_ref[...] = jnp.zeros_like(c_ref)

    def forward(t, s):
        known = isinstance(t, int)
        n = t * SUBS + s
        y_wait(n)
        z_start(n)
        if not known or n + AHEAD <= TOTAL:
            y_start(n + AHEAD)
        if s % WIDE == WIDE - 1:
            m = t * B_SUBS + s // WIDE
            x_wait(m)
            d_start(m)
            if not known or m + B_AHEAD < B_TOTAL:
                x_start(m + B_AHEAD)

    def body(t, carry):
        for s in range(SUBS):
            forward(t, s)
            dt, i = (s - LAG) // SUBS - 1, (s - LAG) % SUBS
            if i % 2 == 0:

                @pl.when(t + dt >= 0)
                def _(dt=dt, i=i):
                    if i == 0:
                        pl.when(t + dt == 0)(wait_local)
                        settle(t + dt)
                    product(t + dt, i // 2)

        return carry

    lax.fori_loop(0, TAIL // SUBS, body, 0)

    work = [(t, p) for t in (STEPS - 4, STEPS - 3, STEPS - 2) for p in range(SUBS // 2)]
    begun = TAIL - (STEPS - 3) * SUBS - LAG
    work = work[(begun + 1) // 2 :]
    for n in range(TAIL, TOTAL):
        forward(n // SUBS, n % SUBS)
        t, p = work[0] if work else (LAST, 0)
        first = (t + 1) * SUBS + LAG
        if t < LAST and n >= first + (2 * p if t < LAST - 1 else p):
            if p == 0:
                settle(t)
            product(t, p)
            work.pop(0)
    for t, p in work:
        if p == 0:
            settle(t)
        product(t, p)
    mine = lanes(2 * (1 - y) + 1 - z)
    early = EARLY * PIECE
    take(b_last.at[lanes(peer_across)], step_sem(dr, LAST))
    take(a_last.at[pl.ds(0, early), mine], zr.at[STEP_RING])
    for i in range(EARLY):
        rows = pl.ds(i * PIECE, PIECE)
        c_ref[rows] += jnp.dot(a_last[rows], b_last[...], preferred_element_type=jnp.float32)
    take(a_last.at[pl.ds(early, SUBS * PIECE - EXTRA - early), mine], step_sem(zr, LAST))
    take(a_last.at[pl.ds(SUBS * PIECE - EXTRA, EXTRA), mine], yr.at[RING])
    take(a_ref, sent.at[0])
    take(b_ref, sent.at[1])


def _finish(c_part, a_last, b_last, c_ref, done, sem):
    early = pl.ds(0, EARLY * PIECE)
    pltpu.make_async_copy(c_part.at[early], c_ref.at[early], sem).start()
    for i in range(EARLY, SUBS):
        rows = pl.ds(i * PIECE, PIECE)
        done[rows] = c_part[rows] + jnp.dot(a_last[rows], b_last[...], preferred_element_type=jnp.float32)
        pltpu.make_async_copy(done.at[rows], c_ref.at[rows], sem).start()
    pltpu.make_async_copy(c_part, c_ref, sem).wait()


def solution(mesh):
    def local_product(a_blk, b_blk):
        rows, half = a_blk.shape
        piece = half // 2
        vmem = pl.BlockSpec(memory_space=pltpu.VMEM)
        hbm = pl.BlockSpec(memory_space=pltpu.HBM)
        parts = pl.pallas_call(
            _exchange,
            out_shape=[
                jax.ShapeDtypeStruct((rows, piece), jnp.float32),
                jax.ShapeDtypeStruct((rows, 4 * CHUNK), jnp.bfloat16),
                jax.ShapeDtypeStruct((4 * CHUNK, piece), jnp.bfloat16),
            ],
            in_specs=[hbm, hbm],
            out_specs=[vmem] * 3,
            scratch_shapes=[
                pltpu.VMEM((LAST, rows, 4 * CHUNK), jnp.bfloat16),
                pltpu.VMEM((LAST, 4 * CHUNK, piece), jnp.bfloat16),
                pltpu.SemaphoreType.DMA((RING + 1,)),
                pltpu.SemaphoreType.DMA((STEP_RING + 1,)),
                pltpu.SemaphoreType.DMA((B_RING,)),
                pltpu.SemaphoreType.DMA((STEP_RING + 1,)),
                pltpu.SemaphoreType.DMA((2,)),
                pltpu.SemaphoreType.DMA((4,)),
                pltpu.SemaphoreType.REGULAR((3,)),
            ],
            compiler_params=pltpu.CompilerParams(collective_id=0, has_side_effects=True, vmem_limit_bytes=LIMIT),
        )(a_blk, b_blk)
        return pl.pallas_call(
            _finish,
            out_shape=jax.ShapeDtypeStruct((rows, piece), jnp.float32),
            in_specs=[vmem] * 3,
            out_specs=hbm,
            scratch_shapes=[pltpu.VMEM((rows, piece), jnp.float32), pltpu.SemaphoreType.DMA],
            compiler_params=pltpu.CompilerParams(vmem_limit_bytes=LIMIT_FINISH),
        )(*parts)

    return jax.shard_map(
        local_product,
        mesh=mesh,
        in_specs=(P("row", "col"), P("row", "col")),
        out_specs=P("row", ("col", "dep")),
        check_vma=False,
    )
```

```python
import jax
import jax.numpy as jnp
from jax import lax
from jax.experimental import pallas as pl
from jax.experimental.pallas import tpu as pltpu
from jax.sharding import PartitionSpec as P

MESH = pl.DeviceIdType.MESH
STEPS = 10
SUBS = 10
CHUNK = 128
PIECE = 128
COLS = 256
TOTAL = STEPS * SUBS
LAST = STEPS - 1
EXTRA = 416
EARLY = 2
AHEAD = 7
WIDE = 5
B_AHEAD = 2
LAG = 6
RING = 2 * AHEAD
B_RING = 2 * B_AHEAD
B_SUBS = SUBS // WIDE
B_TOTAL = STEPS * B_SUBS
STEP_RING = 3
TAIL = (STEPS - 2) * SUBS
LIMIT = 42 * 2**20
LIMIT_FINISH = 20 * 2**20


def _exchange(a_ref, b_ref, c_ref, a_last, b_last, abuf, bbuf, yr, zr, xr, dr, sent, local, ready):
    z, y, r = lax.axis_index("dep"), lax.axis_index("col"), lax.axis_index("row")
    quarter = a_ref.shape[1] // 2
    across = lax.rem(r + 2, 4)
    peer = r + 1 - 2 * lax.rem(r, 2)
    peer_across = lax.rem(peer + 2, 4)
    to_y, to_z, to_x, to_d = {"col": 1 - y}, {"dep": 1 - z}, {"row": across}, {"row": peer}

    def aligned(start, size):
        return pl.ds(pl.multiple_of(start, CHUNK), size)

    def lanes(q):
        return aligned(q * CHUNK, CHUNK)

    def remote(src, dst, send, recv, to):
        return pltpu.make_async_remote_copy(
            src_ref=src, dst_ref=dst, send_sem=send, recv_sem=recv, device_id=to, device_id_type=MESH
        )

    def is_last(t):
        return isinstance(t, int) and t == LAST

    def a_step(t):
        return a_last if is_last(t) else abuf.at[t]

    def b_step(t):
        return b_last if is_last(t) else bbuf.at[t]

    def a_slot(n, q):
        return a_step(n // SUBS).at[aligned((n % SUBS) * PIECE, PIECE), lanes(q)]

    def b_slot(n, q):
        return b_step(n // B_SUBS).at[lanes(q), aligned((n % B_SUBS) * WIDE * PIECE, WIDE * PIECE)]

    def take(some, sem):
        pltpu.make_async_copy(some, some, sem).wait()

    def step_sem(sems, t):
        return sems.at[lax.rem(t, STEP_RING)]

    def y_start(n):
        if isinstance(n, int) and n == TOTAL:
            rows = pl.ds(SUBS * PIECE - EXTRA, EXTRA)
            src = a_ref.at[rows, aligned((1 - z) * quarter + LAST * CHUNK, CHUNK)]
            remote(src, a_last.at[rows, lanes(2 * y + 1 - z)], sent.at[0], yr.at[RING], to_y).start()
            return
        src = a_ref.at[aligned((n % SUBS) * PIECE, PIECE), aligned(z * quarter + n // SUBS * CHUNK, CHUNK)]
        remote(src, a_slot(n, 2 * y + z), sent.at[0], yr.at[lax.rem(n, RING)], to_y).start()

    def y_wait(n):
        take(a_slot(n, 2 * (1 - y) + z), yr.at[lax.rem(n, RING)])

    def z_start(n):
        slot, recv = a_slot(n, 2 * (1 - y) + z), step_sem(zr, n // SUBS)
        if is_last(n // SUBS):
            i = n % SUBS
            size = min(PIECE, SUBS * PIECE - EXTRA - i * PIECE)
            if size <= 0:
                return
            slot = a_last.at[pl.ds(i * PIECE, size), lanes(2 * (1 - y) + z)]
            recv = zr.at[STEP_RING] if i < EARLY else recv
        remote(slot, slot, sent.at[0], recv, to_z).start()

    def x_start(n):
        columns = aligned(z * quarter + (n % B_SUBS) * WIDE * PIECE, WIDE * PIECE)
        src = b_ref.at[aligned(n // B_SUBS * CHUNK, CHUNK), columns]
        remote(src, b_slot(n, r), sent.at[1], xr.at[lax.rem(n, B_RING)], to_x).start()

    def x_wait(n):
        take(b_slot(n, across), xr.at[lax.rem(n, B_RING)])

    def d_start(n):
        slot = b_slot(n, across)
        remote(slot, slot, sent.at[1], step_sem(dr, n // B_SUBS), to_d).start()

    def settle(t):
        take(abuf.at[t, :, lanes(2 * (1 - y) + 1 - z)], step_sem(zr, t))
        take(bbuf.at[t, lanes(peer_across)], step_sem(dr, t))

    def start_local():
        for t in range(STEPS):
            for part in range(2):
                src = a_ref.at[:, pl.ds(part * quarter + t * CHUNK, CHUNK)]
                pltpu.make_async_copy(src, a_step(t).at[:, lanes(2 * y + part)], local.at[0]).start()
            src = b_ref.at[pl.ds(t * CHUNK, CHUNK), aligned(z * quarter, quarter)]
            dst = b_step(t).at[lanes(r)]
            pltpu.make_async_copy(src, dst, local.at[1]).start()

    def start_peer():
        for t in range(STEPS):
            src = b_ref.at[pl.ds(t * CHUNK, CHUNK), aligned(z * quarter, quarter)]
            remote(src, b_step(t).at[lanes(r)], local.at[2], local.at[3], to_d).start()

    def wait_local():
        take(a_ref, local.at[0])
        for i in (1, 2, 3):
            take(b_ref.at[:, pl.ds(0, quarter)], local.at[i])

    def product(t, p):
        cols = pl.ds(p * COLS, COLS)
        c_ref[:, cols] += jnp.dot(abuf[t], bbuf[t, :, cols], preferred_element_type=jnp.float32)

    x, core = r // 2, lax.rem(r, 2)
    axes = ((x, to_x), (y, to_y), (z, to_z), (1 - core, to_d))
    barrier = pltpu.get_barrier_semaphore()
    for at, to in axes:

        @pl.when(at == 0)
        def _(to=to):
            pl.semaphore_signal(barrier, inc=1, device_id=to, device_id_type=MESH)

    ahead = x + y + z + 1 - core
    pl.when(ahead > 0)(lambda: pl.semaphore_wait(barrier, ahead))
    for i, (at, to) in enumerate(axes):

        @pl.when(at == 1)
        def _(i=i, to=to):
            pl.semaphore_signal(ready.at[i], inc=1, device_id=to, device_id_type=MESH)

    def begin(i):
        for n in range((B_AHEAD, AHEAD)[i]):
            (x_start, y_start)[i](n)

    pl.when(y == 1)(lambda: begin(1))
    pl.when(x == 1)(lambda: begin(0))
    start_local()
    pl.when(core == 1)(lambda: pl.semaphore_wait(ready.at[3], 1))
    start_peer()
    for i in (1, 0):

        @pl.when(axes[i][0] == 0)
        def _(i=i):
            pl.semaphore_wait(ready.at[i], 1)
            begin(i)

    pl.when(z == 0)(lambda: pl.semaphore_wait(ready.at[2], 1))
    c_ref[...] = jnp.zeros_like(c_ref)

    def forward(t, s):
        known = isinstance(t, int)
        n = t * SUBS + s
        y_wait(n)
        z_start(n)
        if not known or n + AHEAD <= TOTAL:
            y_start(n + AHEAD)
        if s % WIDE == WIDE - 1:
            m = t * B_SUBS + s // WIDE
            x_wait(m)
            d_start(m)
            if not known or m + B_AHEAD < B_TOTAL:
                x_start(m + B_AHEAD)

    def body(t, carry):
        for s in range(SUBS):
            forward(t, s)
            dt, i = (s - LAG) // SUBS - 1, (s - LAG) % SUBS
            if i % 2 == 0:

                @pl.when(t + dt >= 0)
                def _(dt=dt, i=i):
                    if i == 0:
                        pl.when(t + dt == 0)(wait_local)
                        settle(t + dt)
                    product(t + dt, i // 2)

        return carry

    lax.fori_loop(0, TAIL // SUBS, body, 0)

    work = [(t, p) for t in (STEPS - 4, STEPS - 3, STEPS - 2) for p in range(SUBS // 2)]
    begun = TAIL - (STEPS - 3) * SUBS - LAG
    work = work[(begun + 1) // 2 :]
    for n in range(TAIL, TOTAL):
        forward(n // SUBS, n % SUBS)
        t, p = work[0] if work else (LAST, 0)
        first = (t + 1) * SUBS + LAG
        if t < LAST and n >= first + (2 * p if t < LAST - 1 else p):
            if p == 0:
                settle(t)
            product(t, p)
            work.pop(0)
    for t, p in work:
        if p == 0:
            settle(t)
        product(t, p)
    mine = lanes(2 * (1 - y) + 1 - z)
    early = EARLY * PIECE
    take(b_last.at[lanes(peer_across)], step_sem(dr, LAST))
    take(a_last.at[pl.ds(0, early), mine], zr.at[STEP_RING])
    for i in range(EARLY):
        rows = pl.ds(i * PIECE, PIECE)
        c_ref[rows] += jnp.dot(a_last[rows], b_last[...], preferred_element_type=jnp.float32)
    take(a_last.at[pl.ds(early, SUBS * PIECE - EXTRA - early), mine], step_sem(zr, LAST))
    take(a_last.at[pl.ds(SUBS * PIECE - EXTRA, EXTRA), mine], yr.at[RING])
    take(a_ref, sent.at[0])
    take(b_ref, sent.at[1])


def _finish(c_part, a_last, b_last, c_ref, done, sem):
    early = pl.ds(0, EARLY * PIECE)
    pltpu.make_async_copy(c_part.at[early], c_ref.at[early], sem).start()
    for i in range(EARLY, SUBS):
        rows = pl.ds(i * PIECE, PIECE)
        done[rows] = c_part[rows] + jnp.dot(a_last[rows], b_last[...], preferred_element_type=jnp.float32)
        pltpu.make_async_copy(done.at[rows], c_ref.at[rows], sem).start()
    pltpu.make_async_copy(c_part, c_ref, sem).wait()


def solution(mesh):
    def local_product(a_blk, b_blk):
        rows, half = a_blk.shape
        piece = half // 2
        vmem = pl.BlockSpec(memory_space=pltpu.VMEM)
        hbm = pl.BlockSpec(memory_space=pltpu.HBM)
        parts = pl.pallas_call(
            _exchange,
            out_shape=[
                jax.ShapeDtypeStruct((rows, piece), jnp.float32),
                jax.ShapeDtypeStruct((rows, 4 * CHUNK), jnp.bfloat16),
                jax.ShapeDtypeStruct((4 * CHUNK, piece), jnp.bfloat16),
            ],
            in_specs=[hbm, hbm],
            out_specs=[vmem] * 3,
            scratch_shapes=[
                pltpu.VMEM((LAST, rows, 4 * CHUNK), jnp.bfloat16),
                pltpu.VMEM((LAST, 4 * CHUNK, piece), jnp.bfloat16),
                pltpu.SemaphoreType.DMA((RING + 1,)),
                pltpu.SemaphoreType.DMA((STEP_RING + 1,)),
                pltpu.SemaphoreType.DMA((B_RING,)),
                pltpu.SemaphoreType.DMA((STEP_RING + 1,)),
                pltpu.SemaphoreType.DMA((2,)),
                pltpu.SemaphoreType.DMA((4,)),
                pltpu.SemaphoreType.REGULAR((4,)),
            ],
            compiler_params=pltpu.CompilerParams(collective_id=0, has_side_effects=True, vmem_limit_bytes=LIMIT),
        )(a_blk, b_blk)
        return pl.pallas_call(
            _finish,
            out_shape=jax.ShapeDtypeStruct((rows, piece), jnp.float32),
            in_specs=[vmem] * 3,
            out_specs=hbm,
            scratch_shapes=[pltpu.VMEM((rows, piece), jnp.float32), pltpu.SemaphoreType.DMA],
            compiler_params=pltpu.CompilerParams(vmem_limit_bytes=LIMIT_FINISH),
        )(*parts)

    return jax.shard_map(
        local_product,
        mesh=mesh,
        in_specs=(P("row", "col"), P("row", "col")),
        out_specs=P("row", ("col", "dep")),
        check_vma=False,
    )
```

```python
import jax
import jax.numpy as jnp
from jax import lax
from jax.experimental import pallas as pl
from jax.experimental.pallas import tpu as pltpu
from jax.sharding import PartitionSpec as P

MESH = pl.DeviceIdType.MESH
STEPS = 10
SUBS = 10
CHUNK = 128
PIECE = 128
COLS = 256
TOTAL = STEPS * SUBS
LAST = STEPS - 1
EXTRA = 448
EARLY = 2
AHEAD = 7
WIDE = 5
B_AHEAD = 2
FIRST_HALF = (91, 93, 95, 97, 97)
SECOND_HALF = (97, 98, 98, 99, 99)
LAG = 6
RING = 2 * AHEAD
B_RING = 2 * B_AHEAD
B_SUBS = SUBS // WIDE
B_TOTAL = STEPS * B_SUBS
STEP_RING = 3
TAIL = (STEPS - 2) * SUBS
LIMIT = 42 * 2**20
LIMIT_FINISH = 20 * 2**20


def _exchange(a_ref, b_ref, c_ref, a_last, b_last, abuf, bbuf, yr, zr, xr, dr, sent, local, ready):
    z, y, r = lax.axis_index("dep"), lax.axis_index("col"), lax.axis_index("row")
    quarter = a_ref.shape[1] // 2
    across = lax.rem(r + 2, 4)
    peer = r + 1 - 2 * lax.rem(r, 2)
    peer_across = lax.rem(peer + 2, 4)
    to_y, to_z, to_x, to_d = {"col": 1 - y}, {"dep": 1 - z}, {"row": across}, {"row": peer}

    def aligned(start, size):
        return pl.ds(pl.multiple_of(start, CHUNK), size)

    def lanes(q):
        return aligned(q * CHUNK, CHUNK)

    def remote(src, dst, send, recv, to):
        return pltpu.make_async_remote_copy(
            src_ref=src, dst_ref=dst, send_sem=send, recv_sem=recv, device_id=to, device_id_type=MESH
        )

    def is_last(t):
        return isinstance(t, int) and t == LAST

    def a_step(t):
        return a_last if is_last(t) else abuf.at[t]

    def b_step(t):
        return b_last if is_last(t) else bbuf.at[t]

    def a_slot(n, q):
        return a_step(n // SUBS).at[aligned((n % SUBS) * PIECE, PIECE), lanes(q)]

    def b_slot(n, q):
        return b_step(n // B_SUBS).at[lanes(q), aligned((n % B_SUBS) * WIDE * PIECE, WIDE * PIECE)]

    def take(some, sem):
        pltpu.make_async_copy(some, some, sem).wait()

    def step_sem(sems, t):
        return sems.at[lax.rem(t, STEP_RING)]

    def y_start(n):
        if isinstance(n, int) and n == TOTAL:
            rows = pl.ds(SUBS * PIECE - EXTRA, EXTRA)
            src = a_ref.at[rows, aligned((1 - z) * quarter + LAST * CHUNK, CHUNK)]
            remote(src, a_last.at[rows, lanes(2 * y + 1 - z)], sent.at[0], yr.at[RING], to_y).start()
            return
        src = a_ref.at[aligned((n % SUBS) * PIECE, PIECE), aligned(z * quarter + n // SUBS * CHUNK, CHUNK)]
        remote(src, a_slot(n, 2 * y + z), sent.at[0], yr.at[lax.rem(n, RING)], to_y).start()

    def y_wait(n):
        take(a_slot(n, 2 * (1 - y) + z), yr.at[lax.rem(n, RING)])

    def z_start(n):
        slot, recv = a_slot(n, 2 * (1 - y) + z), step_sem(zr, n // SUBS)
        if is_last(n // SUBS):
            i = n % SUBS
            size = min(PIECE, SUBS * PIECE - EXTRA - i * PIECE)
            if size <= 0:
                return
            slot = a_last.at[pl.ds(i * PIECE, size), lanes(2 * (1 - y) + z)]
            recv = zr.at[STEP_RING] if i < EARLY else recv
        remote(slot, slot, sent.at[0], recv, to_z).start()

    def x_start(n):
        columns = aligned(z * quarter + (n % B_SUBS) * WIDE * PIECE, WIDE * PIECE)
        src = b_ref.at[aligned(n // B_SUBS * CHUNK, CHUNK), columns]
        remote(src, b_slot(n, r), sent.at[1], xr.at[lax.rem(n, B_RING)], to_x).start()

    def x_wait(n):
        take(b_slot(n, across), xr.at[lax.rem(n, B_RING)])

    def d_start(n):
        slot = b_slot(n, across)
        remote(slot, slot, sent.at[1], step_sem(dr, n // B_SUBS), to_d).start()

    def settle(t):
        take(abuf.at[t, :, lanes(2 * (1 - y) + 1 - z)], step_sem(zr, t))
        take(bbuf.at[t, lanes(peer_across)], step_sem(dr, t))

    def start_local():
        for t in range(STEPS):
            for part in range(2):
                src = a_ref.at[:, pl.ds(part * quarter + t * CHUNK, CHUNK)]
                pltpu.make_async_copy(src, a_step(t).at[:, lanes(2 * y + part)], local.at[0]).start()
            src = b_ref.at[pl.ds(t * CHUNK, CHUNK), aligned(z * quarter, quarter)]
            dst = b_step(t).at[lanes(r)]
            pltpu.make_async_copy(src, dst, local.at[1]).start()

    def start_peer():
        for t in range(STEPS):
            src = b_ref.at[pl.ds(t * CHUNK, CHUNK), aligned(z * quarter, quarter)]
            remote(src, b_step(t).at[lanes(r)], local.at[2], local.at[3], to_d).start()

    def wait_local():
        take(a_ref, local.at[0])
        for i in (1, 2, 3):
            take(b_ref.at[:, pl.ds(0, quarter)], local.at[i])

    def product(t, p):
        cols = pl.ds(p * COLS, COLS)
        c_ref[:, cols] += jnp.dot(abuf[t], bbuf[t, :, cols], preferred_element_type=jnp.float32)

    x, core = r // 2, lax.rem(r, 2)
    axes = ((x, to_x), (y, to_y), (z, to_z), (1 - core, to_d))
    def half_product(t, p, side):
        cols, half = pl.ds(p * COLS, COLS), aligned(side * 2 * CHUNK, 2 * CHUNK)
        c_ref[:, cols] += jnp.dot(abuf[t, :, half], bbuf[t, half, cols], preferred_element_type=jnp.float32)

    barrier = pltpu.get_barrier_semaphore()
    for at, to in axes:

        @pl.when(at == 0)
        def _(to=to):
            pl.semaphore_signal(barrier, inc=1, device_id=to, device_id_type=MESH)

    ahead = x + y + z + 1 - core
    pl.when(ahead > 0)(lambda: pl.semaphore_wait(barrier, ahead))
    for i, (at, to) in enumerate(axes):

        @pl.when(at == 1)
        def _(i=i, to=to):
            pl.semaphore_signal(ready.at[i], inc=1, device_id=to, device_id_type=MESH)

    def begin(i):
        for n in range((B_AHEAD, AHEAD)[i]):
            (x_start, y_start)[i](n)

    pl.when(y == 1)(lambda: begin(1))
    pl.when(x == 1)(lambda: begin(0))
    start_local()
    pl.when(core == 1)(lambda: pl.semaphore_wait(ready.at[3], 1))
    start_peer()
    for i in (1, 0):

        @pl.when(axes[i][0] == 0)
        def _(i=i):
            pl.semaphore_wait(ready.at[i], 1)
            begin(i)

    pl.when(z == 0)(lambda: pl.semaphore_wait(ready.at[2], 1))
    c_ref[...] = jnp.zeros_like(c_ref)

    def forward(t, s):
        known = isinstance(t, int)
        n = t * SUBS + s
        y_wait(n)
        z_start(n)
        if not known or n + AHEAD <= TOTAL:
            y_start(n + AHEAD)
        if s % WIDE == WIDE - 1:
            m = t * B_SUBS + s // WIDE
            x_wait(m)
            d_start(m)
            if not known or m + B_AHEAD < B_TOTAL:
                x_start(m + B_AHEAD)

    def body(t, carry):
        for s in range(SUBS):
            forward(t, s)
            dt, i = (s - LAG) // SUBS - 1, (s - LAG) % SUBS
            if i % 2 == 0:

                @pl.when(t + dt >= 0)
                def _(dt=dt, i=i):
                    if i == 0:
                        pl.when(t + dt == 0)(wait_local)
                        settle(t + dt)
                    product(t + dt, i // 2)

        return carry

    lax.fori_loop(0, TAIL // SUBS, body, 0)

    prior = LAST - 1
    work = {}
    for t in (prior - 2, prior - 1):
        for p in range(SUBS // 2):
            work.setdefault((t + 1) * SUBS + LAG + 2 * p, []).append((t, p, None))
    for p in range(SUBS // 2):
        work.setdefault(FIRST_HALF[p], []).append((prior, p, 0))
        work.setdefault(SECOND_HALF[p], []).append((prior, p, 1))
    for n in range(TAIL, TOTAL):
        forward(n // SUBS, n % SUBS)
        for t, p, half in work.get(n, ()):
            if half is None:
                if p == 0:
                    settle(t)
                product(t, p)
                continue
            if p == 0 and half == 0:
                take(bbuf.at[t, lanes(peer_across)], step_sem(dr, t))
            if p == 0 and half == 1:
                take(abuf.at[t, :, lanes(2 * (1 - y) + 1 - z)], step_sem(zr, t))
            half_product(t, p, (y, 1 - y)[half])
    mine = lanes(2 * (1 - y) + 1 - z)
    early = EARLY * PIECE
    take(b_last.at[lanes(peer_across)], step_sem(dr, LAST))
    take(a_last.at[pl.ds(0, early), mine], zr.at[STEP_RING])
    for i in range(EARLY):
        rows = pl.ds(i * PIECE, PIECE)
        c_ref[rows] += jnp.dot(a_last[rows], b_last[...], preferred_element_type=jnp.float32)
    take(a_last.at[pl.ds(early, SUBS * PIECE - EXTRA - early), mine], step_sem(zr, LAST))
    take(a_last.at[pl.ds(SUBS * PIECE - EXTRA, EXTRA), mine], yr.at[RING])
    take(a_ref, sent.at[0])
    take(b_ref, sent.at[1])


def _finish(c_part, a_last, b_last, c_ref, done, sem):
    early = pl.ds(0, EARLY * PIECE)
    pltpu.make_async_copy(c_part.at[early], c_ref.at[early], sem).start()
    for i in range(EARLY, SUBS):
        rows = pl.ds(i * PIECE, PIECE)
        done[rows] = c_part[rows] + jnp.dot(a_last[rows], b_last[...], preferred_element_type=jnp.float32)
        pltpu.make_async_copy(done.at[rows], c_ref.at[rows], sem).start()
    pltpu.make_async_copy(c_part, c_ref, sem).wait()


def solution(mesh):
    def local_product(a_blk, b_blk):
        rows, half = a_blk.shape
        piece = half // 2
        vmem = pl.BlockSpec(memory_space=pltpu.VMEM)
        hbm = pl.BlockSpec(memory_space=pltpu.HBM)
        parts = pl.pallas_call(
            _exchange,
            out_shape=[
                jax.ShapeDtypeStruct((rows, piece), jnp.float32),
                jax.ShapeDtypeStruct((rows, 4 * CHUNK), jnp.bfloat16),
                jax.ShapeDtypeStruct((4 * CHUNK, piece), jnp.bfloat16),
            ],
            in_specs=[hbm, hbm],
            out_specs=[vmem] * 3,
            scratch_shapes=[
                pltpu.VMEM((LAST, rows, 4 * CHUNK), jnp.bfloat16),
                pltpu.VMEM((LAST, 4 * CHUNK, piece), jnp.bfloat16),
                pltpu.SemaphoreType.DMA((RING + 1,)),
                pltpu.SemaphoreType.DMA((STEP_RING + 1,)),
                pltpu.SemaphoreType.DMA((B_RING,)),
                pltpu.SemaphoreType.DMA((STEP_RING + 1,)),
                pltpu.SemaphoreType.DMA((2,)),
                pltpu.SemaphoreType.DMA((4,)),
                pltpu.SemaphoreType.REGULAR((4,)),
            ],
            compiler_params=pltpu.CompilerParams(collective_id=0, has_side_effects=True, vmem_limit_bytes=LIMIT),
        )(a_blk, b_blk)
        return pl.pallas_call(
            _finish,
            out_shape=jax.ShapeDtypeStruct((rows, piece), jnp.float32),
            in_specs=[vmem] * 3,
            out_specs=hbm,
            scratch_shapes=[pltpu.VMEM((rows, piece), jnp.float32), pltpu.SemaphoreType.DMA],
            compiler_params=pltpu.CompilerParams(vmem_limit_bytes=LIMIT_FINISH),
        )(*parts)

    return jax.shard_map(
        local_product,
        mesh=mesh,
        in_specs=(P("row", "col"), P("row", "col")),
        out_specs=P("row", ("col", "dep")),
        check_vma=False,
    )
```

```python
import jax
import jax.numpy as jnp
from jax import lax
from jax.experimental import pallas as pl
from jax.experimental.pallas import tpu as pltpu
from jax.sharding import PartitionSpec as P

MESH = pl.DeviceIdType.MESH
STEPS = 10
SUBS = 10
CHUNK = 128
PIECE = 128
COLS = 256
TOTAL = STEPS * SUBS
LAST = STEPS - 1
EXTRA = 448
EARLY = 2
AHEAD = 7
WIDE = 5
B_AHEAD = 2
FIRST_HALF = (91, 93, 95, 97, 97)
SECOND_HALF = (97, 98, 98, 99, 99)
LAG = 6
RING = 2 * AHEAD
B_RING = 2 * B_AHEAD
B_SUBS = SUBS // WIDE
B_TOTAL = STEPS * B_SUBS
STEP_RING = 3
TAIL = (STEPS - 2) * SUBS
LIMIT = 42 * 2**20
LIMIT_FINISH = 20 * 2**20


def _exchange(a_ref, b_ref, c_ref, a_last, b_last, abuf, bbuf, yr, zr, xr, dr, sent, local, ready):
    z, y, r = lax.axis_index("dep"), lax.axis_index("col"), lax.axis_index("row")
    quarter = a_ref.shape[1] // 2
    across = lax.rem(r + 2, 4)
    peer = r + 1 - 2 * lax.rem(r, 2)
    peer_across = lax.rem(peer + 2, 4)
    to_y, to_z, to_x, to_d = {"col": 1 - y}, {"dep": 1 - z}, {"row": across}, {"row": peer}

    def aligned(start, size):
        return pl.ds(pl.multiple_of(start, CHUNK), size)

    def lanes(q):
        return aligned(q * CHUNK, CHUNK)

    def remote(src, dst, send, recv, to):
        return pltpu.make_async_remote_copy(
            src_ref=src, dst_ref=dst, send_sem=send, recv_sem=recv, device_id=to, device_id_type=MESH
        )

    def is_last(t):
        return isinstance(t, int) and t == LAST

    def a_step(t):
        return a_last if is_last(t) else abuf.at[t]

    def b_step(t):
        return b_last if is_last(t) else bbuf.at[t]

    def a_slot(n, q):
        return a_step(n // SUBS).at[aligned((n % SUBS) * PIECE, PIECE), lanes(q)]

    def b_slot(n, q):
        return b_step(n // B_SUBS).at[lanes(q), aligned((n % B_SUBS) * WIDE * PIECE, WIDE * PIECE)]

    def take(some, sem):
        pltpu.make_async_copy(some, some, sem).wait()

    def step_sem(sems, t):
        return sems.at[lax.rem(t, STEP_RING)]

    def y_start(n):
        if isinstance(n, int) and n == TOTAL:
            rows = pl.ds(SUBS * PIECE - EXTRA, EXTRA)
            src = a_ref.at[rows, aligned((1 - z) * quarter + LAST * CHUNK, CHUNK)]
            remote(src, a_last.at[rows, lanes(2 * y + 1 - z)], sent.at[0], yr.at[RING], to_y).start()
            return
        src = a_ref.at[aligned((n % SUBS) * PIECE, PIECE), aligned(z * quarter + n // SUBS * CHUNK, CHUNK)]
        remote(src, a_slot(n, 2 * y + z), sent.at[0], yr.at[lax.rem(n, RING)], to_y).start()

    def y_wait(n):
        take(a_slot(n, 2 * (1 - y) + z), yr.at[lax.rem(n, RING)])

    def z_start(n):
        slot, recv = a_slot(n, 2 * (1 - y) + z), step_sem(zr, n // SUBS)
        if is_last(n // SUBS):
            i = n % SUBS
            size = min(PIECE, SUBS * PIECE - EXTRA - i * PIECE)
            if size <= 0:
                return
            slot = a_last.at[pl.ds(i * PIECE, size), lanes(2 * (1 - y) + z)]
            recv = zr.at[STEP_RING] if i < EARLY else recv
        remote(slot, slot, sent.at[0], recv, to_z).start()

    def x_start(n):
        columns = aligned(z * quarter + (n % B_SUBS) * WIDE * PIECE, WIDE * PIECE)
        src = b_ref.at[aligned(n // B_SUBS * CHUNK, CHUNK), columns]
        remote(src, b_slot(n, r), sent.at[1], xr.at[lax.rem(n, B_RING)], to_x).start()

    def x_wait(n):
        take(b_slot(n, across), xr.at[lax.rem(n, B_RING)])

    def d_start(n):
        slot = b_slot(n, across)
        remote(slot, slot, sent.at[1], step_sem(dr, n // B_SUBS), to_d).start()

    def settle(t):
        take(abuf.at[t, :, lanes(2 * (1 - y) + 1 - z)], step_sem(zr, t))
        take(bbuf.at[t, lanes(peer_across)], step_sem(dr, t))

    def start_local():
        for t in range(STEPS):
            for part in range(2):
                src = a_ref.at[:, pl.ds(part * quarter + t * CHUNK, CHUNK)]
                pltpu.make_async_copy(src, a_step(t).at[:, lanes(2 * y + part)], local.at[0]).start()
            src = b_ref.at[pl.ds(t * CHUNK, CHUNK), aligned(z * quarter, quarter)]
            dst = b_step(t).at[lanes(r)]
            pltpu.make_async_copy(src, dst, local.at[0]).start()

    def start_peer():
        for t in range(STEPS):
            src = b_ref.at[pl.ds(t * CHUNK, CHUNK), aligned(z * quarter, quarter)]
            remote(src, b_step(t).at[lanes(r)], sent.at[1], local.at[1], to_d).start()

    def wait_local():
        take(abuf.at[pl.ds(0, 8), pl.ds(0, 1200)], local.at[0])
        take(b_ref.at[:, pl.ds(0, quarter)], local.at[1])

    def product(t, p):
        cols = pl.ds(p * COLS, COLS)
        c_ref[:, cols] += jnp.dot(abuf[t], bbuf[t, :, cols], preferred_element_type=jnp.float32)

    x, core = r // 2, lax.rem(r, 2)
    axes = ((x, to_x), (y, to_y), (z, to_z), (1 - core, to_d))
    def half_product(t, p, side):
        cols, half = pl.ds(p * COLS, COLS), aligned(side * 2 * CHUNK, 2 * CHUNK)
        c_ref[:, cols] += jnp.dot(abuf[t, :, half], bbuf[t, half, cols], preferred_element_type=jnp.float32)

    barrier = pltpu.get_barrier_semaphore()
    for at, to in axes:

        @pl.when(at == 0)
        def _(to=to):
            pl.semaphore_signal(barrier, inc=1, device_id=to, device_id_type=MESH)

    ahead = x + y + z + 1 - core
    pl.when(ahead > 0)(lambda: pl.semaphore_wait(barrier, ahead))
    for i, (at, to) in enumerate(axes):

        @pl.when(at == 1)
        def _(i=i, to=to):
            pl.semaphore_signal(ready.at[i], inc=1, device_id=to, device_id_type=MESH)

    def begin(i):
        for n in range((B_AHEAD, AHEAD)[i]):
            (x_start, y_start)[i](n)

    pl.when(y == 1)(lambda: begin(1))
    pl.when(x == 1)(lambda: begin(0))
    start_local()
    pl.when(core == 1)(lambda: pl.semaphore_wait(ready.at[3], 1))
    start_peer()
    for i in (1, 0):

        @pl.when(axes[i][0] == 0)
        def _(i=i):
            pl.semaphore_wait(ready.at[i], 1)
            begin(i)

    pl.when(z == 0)(lambda: pl.semaphore_wait(ready.at[2], 1))
    c_ref[...] = jnp.zeros_like(c_ref)

    def forward(t, s):
        known = isinstance(t, int)
        n = t * SUBS + s
        y_wait(n)
        z_start(n)
        if not known or n + AHEAD <= TOTAL:
            y_start(n + AHEAD)
        if s % WIDE == WIDE - 1:
            m = t * B_SUBS + s // WIDE
            x_wait(m)
            d_start(m)
            if not known or m + B_AHEAD < B_TOTAL:
                x_start(m + B_AHEAD)

    def body(t, carry):
        for s in range(SUBS):
            forward(t, s)
            dt, i = (s - LAG) // SUBS - 1, (s - LAG) % SUBS
            if i % 2 == 0:

                @pl.when(t + dt >= 0)
                def _(dt=dt, i=i):
                    if i == 0:
                        pl.when(t + dt == 0)(wait_local)
                        settle(t + dt)
                    product(t + dt, i // 2)

        return carry

    lax.fori_loop(0, TAIL // SUBS, body, 0)

    prior = LAST - 1
    work = {}
    for t in (prior - 2, prior - 1):
        for p in range(SUBS // 2):
            work.setdefault((t + 1) * SUBS + LAG + 2 * p, []).append((t, p, None))
    for p in range(SUBS // 2):
        work.setdefault(FIRST_HALF[p], []).append((prior, p, 0))
        work.setdefault(SECOND_HALF[p], []).append((prior, p, 1))
    for n in range(TAIL, TOTAL):
        forward(n // SUBS, n % SUBS)
        for t, p, half in work.get(n, ()):
            if half is None:
                if p == 0:
                    settle(t)
                product(t, p)
                continue
            if p == 0 and half == 0:
                take(bbuf.at[t, lanes(peer_across)], step_sem(dr, t))
            if p == 0 and half == 1:
                take(abuf.at[t, :, lanes(2 * (1 - y) + 1 - z)], step_sem(zr, t))
            half_product(t, p, (y, 1 - y)[half])
    mine = lanes(2 * (1 - y) + 1 - z)
    early = EARLY * PIECE
    take(b_last.at[lanes(peer_across)], step_sem(dr, LAST))
    take(a_last.at[pl.ds(0, early), mine], zr.at[STEP_RING])
    for i in range(EARLY):
        rows = pl.ds(i * PIECE, PIECE)
        c_ref[rows] += jnp.dot(a_last[rows], b_last[...], preferred_element_type=jnp.float32)
    take(a_last.at[pl.ds(early, SUBS * PIECE - EXTRA - early), mine], step_sem(zr, LAST))
    take(a_last.at[pl.ds(SUBS * PIECE - EXTRA, EXTRA), mine], yr.at[RING])
    take(a_ref, sent.at[0])
    take(abuf.at[pl.ds(0, 8), pl.ds(0, 1200)], sent.at[1])


def _finish(c_part, a_last, b_last, c_ref, done, sem):
    early = pl.ds(0, EARLY * PIECE)
    pltpu.make_async_copy(c_part.at[early], c_ref.at[early], sem).start()
    for i in range(EARLY, SUBS):
        rows = pl.ds(i * PIECE, PIECE)
        done[rows] = c_part[rows] + jnp.dot(a_last[rows], b_last[...], preferred_element_type=jnp.float32)
        pltpu.make_async_copy(done.at[rows], c_ref.at[rows], sem).start()
    pltpu.make_async_copy(c_part, c_ref, sem).wait()


def solution(mesh):
    def local_product(a_blk, b_blk):
        rows, half = a_blk.shape
        piece = half // 2
        vmem = pl.BlockSpec(memory_space=pltpu.VMEM)
        hbm = pl.BlockSpec(memory_space=pltpu.HBM)
        parts = pl.pallas_call(
            _exchange,
            out_shape=[
                jax.ShapeDtypeStruct((rows, piece), jnp.float32),
                jax.ShapeDtypeStruct((rows, 4 * CHUNK), jnp.bfloat16),
                jax.ShapeDtypeStruct((4 * CHUNK, piece), jnp.bfloat16),
            ],
            in_specs=[hbm, hbm],
            out_specs=[vmem] * 3,
            scratch_shapes=[
                pltpu.VMEM((LAST, rows, 4 * CHUNK), jnp.bfloat16),
                pltpu.VMEM((LAST, 4 * CHUNK, piece), jnp.bfloat16),
                pltpu.SemaphoreType.DMA((RING + 1,)),
                pltpu.SemaphoreType.DMA((STEP_RING + 1,)),
                pltpu.SemaphoreType.DMA((B_RING,)),
                pltpu.SemaphoreType.DMA((STEP_RING + 1,)),
                pltpu.SemaphoreType.DMA((2,)),
                pltpu.SemaphoreType.DMA((2,)),
                pltpu.SemaphoreType.REGULAR((4,)),
            ],
            compiler_params=pltpu.CompilerParams(collective_id=0, has_side_effects=True, vmem_limit_bytes=LIMIT),
        )(a_blk, b_blk)
        return pl.pallas_call(
            _finish,
            out_shape=jax.ShapeDtypeStruct((rows, piece), jnp.float32),
            in_specs=[vmem] * 3,
            out_specs=hbm,
            scratch_shapes=[pltpu.VMEM((rows, piece), jnp.float32), pltpu.SemaphoreType.DMA],
            compiler_params=pltpu.CompilerParams(vmem_limit_bytes=LIMIT_FINISH),
        )(*parts)

    return jax.shard_map(
        local_product,
        mesh=mesh,
        in_specs=(P("row", "col"), P("row", "col")),
        out_specs=P("row", ("col", "dep")),
        check_vma=False,
    )
```

```python
import jax
import jax.numpy as jnp
from jax import lax
from jax.experimental import pallas as pl
from jax.experimental.pallas import tpu as pltpu
from jax.sharding import PartitionSpec as P

MESH = pl.DeviceIdType.MESH
STEPS = 10
SUBS = 10
CHUNK = 128
PIECE = 128
COLS = 256
TOTAL = STEPS * SUBS
LAST = STEPS - 1
EXTRA = 448
EARLY = 2
AHEAD = 7
WIDE = 5
B_AHEAD = 2
FIRST_HALF = (91, 93, 95, 97, 97)
SECOND_HALF = (97, 98, 98, 99, 99)
LAG = 6
RING = 2 * AHEAD
B_RING = 2 * B_AHEAD
B_SUBS = SUBS // WIDE
B_TOTAL = STEPS * B_SUBS
STEP_RING = 3
TAIL = (STEPS - 2) * SUBS
LIMIT = 42 * 2**20
LIMIT_FINISH = 20 * 2**20


def _exchange(a_ref, b_ref, c_ref, a_last, b_last, abuf, bbuf, yr, zr, xr, dr, sent, local, ready):
    z, y, r = lax.axis_index("dep"), lax.axis_index("col"), lax.axis_index("row")
    quarter = a_ref.shape[1] // 2
    across = lax.rem(r + 2, 4)
    peer = r + 1 - 2 * lax.rem(r, 2)
    peer_across = lax.rem(peer + 2, 4)
    to_y, to_z, to_x, to_d = {"col": 1 - y}, {"dep": 1 - z}, {"row": across}, {"row": peer}

    def aligned(start, size):
        return pl.ds(pl.multiple_of(start, CHUNK), size)

    def lanes(q):
        return aligned(q * CHUNK, CHUNK)

    def remote(src, dst, send, recv, to):
        return pltpu.make_async_remote_copy(
            src_ref=src, dst_ref=dst, send_sem=send, recv_sem=recv, device_id=to, device_id_type=MESH
        )

    def is_last(t):
        return isinstance(t, int) and t == LAST

    def a_step(t):
        return a_last if is_last(t) else abuf.at[t]

    def b_step(t):
        return b_last if is_last(t) else bbuf.at[t]

    def a_slot(n, q):
        return a_step(n // SUBS).at[aligned((n % SUBS) * PIECE, PIECE), lanes(q)]

    def b_slot(n, q):
        return b_step(n // B_SUBS).at[lanes(q), aligned((n % B_SUBS) * WIDE * PIECE, WIDE * PIECE)]

    def take(some, sem):
        pltpu.make_async_copy(some, some, sem).wait()

    def step_sem(sems, t):
        return sems.at[lax.rem(t, STEP_RING)]

    def y_start(n):
        if isinstance(n, int) and n == TOTAL:
            rows = pl.ds(SUBS * PIECE - EXTRA, EXTRA)
            src = a_ref.at[rows, aligned((1 - z) * quarter + LAST * CHUNK, CHUNK)]
            remote(src, a_last.at[rows, lanes(2 * y + 1 - z)], sent.at[0], step_sem(zr, LAST), to_y).start()
            return
        src = a_ref.at[aligned((n % SUBS) * PIECE, PIECE), aligned(z * quarter + n // SUBS * CHUNK, CHUNK)]
        remote(src, a_slot(n, 2 * y + z), sent.at[0], yr.at[lax.rem(n, RING)], to_y).start()

    def y_wait(n):
        take(a_slot(n, 2 * (1 - y) + z), yr.at[lax.rem(n, RING)])

    def z_start(n):
        slot, recv = a_slot(n, 2 * (1 - y) + z), step_sem(zr, n // SUBS)
        if is_last(n // SUBS):
            i = n % SUBS
            size = min(PIECE, SUBS * PIECE - EXTRA - i * PIECE)
            if size <= 0:
                return
            slot = a_last.at[pl.ds(i * PIECE, size), lanes(2 * (1 - y) + z)]
            recv = zr.at[STEP_RING] if i < EARLY else recv
        remote(slot, slot, sent.at[0], recv, to_z).start()

    def x_start(n):
        columns = aligned(z * quarter + (n % B_SUBS) * WIDE * PIECE, WIDE * PIECE)
        src = b_ref.at[aligned(n // B_SUBS * CHUNK, CHUNK), columns]
        remote(src, b_slot(n, r), sent.at[1], xr.at[lax.rem(n, B_RING)], to_x).start()

    def x_wait(n):
        take(b_slot(n, across), xr.at[lax.rem(n, B_RING)])

    def d_start(n):
        slot = b_slot(n, across)
        t = n // B_SUBS
        remote(slot, slot, sent.at[1], zr.at[STEP_RING] if is_last(t) else step_sem(dr, t), to_d).start()

    def settle(t):
        take(abuf.at[t, :, lanes(2 * (1 - y) + 1 - z)], step_sem(zr, t))
        take(bbuf.at[t, lanes(peer_across)], step_sem(dr, t))

    def start_local():
        for t in range(STEPS):
            for part in range(2):
                src = a_ref.at[:, pl.ds(part * quarter + t * CHUNK, CHUNK)]
                pltpu.make_async_copy(src, a_step(t).at[:, lanes(2 * y + part)], local.at[0]).start()
            src = b_ref.at[pl.ds(t * CHUNK, CHUNK), aligned(z * quarter, quarter)]
            dst = b_step(t).at[lanes(r)]
            pltpu.make_async_copy(src, dst, local.at[0]).start()

    def start_peer():
        for t in range(STEPS):
            src = b_ref.at[pl.ds(t * CHUNK, CHUNK), aligned(z * quarter, quarter)]
            remote(src, b_step(t).at[lanes(r)], sent.at[1], local.at[1], to_d).start()

    def wait_local():
        take(abuf.at[pl.ds(0, 8), pl.ds(0, 1200)], local.at[0])
        take(b_ref.at[:, pl.ds(0, quarter)], local.at[1])

    def product(t, p):
        cols = pl.ds(p * COLS, COLS)
        c_ref[:, cols] += jnp.dot(abuf[t], bbuf[t, :, cols], preferred_element_type=jnp.float32)

    x, core = r // 2, lax.rem(r, 2)
    axes = ((x, to_x), (y, to_y), (z, to_z), (1 - core, to_d))
    def half_product(t, p, side):
        cols, half = pl.ds(p * COLS, COLS), aligned(side * 2 * CHUNK, 2 * CHUNK)
        c_ref[:, cols] += jnp.dot(abuf[t, :, half], bbuf[t, half, cols], preferred_element_type=jnp.float32)

    barrier = pltpu.get_barrier_semaphore()
    for at, to in axes:

        @pl.when(at == 0)
        def _(to=to):
            pl.semaphore_signal(barrier, inc=1, device_id=to, device_id_type=MESH)

    ahead = x + y + z + 1 - core
    pl.when(ahead > 0)(lambda: pl.semaphore_wait(barrier, ahead))
    for i, (at, to) in enumerate(axes):

        @pl.when(at == 1)
        def _(i=i, to=to):
            pl.semaphore_signal(ready.at[i], inc=1, device_id=to, device_id_type=MESH)

    def begin(i):
        for n in range((B_AHEAD, AHEAD)[i]):
            (x_start, y_start)[i](n)

    pl.when(y == 1)(lambda: begin(1))
    pl.when(x == 1)(lambda: begin(0))
    start_local()
    pl.when(core == 1)(lambda: pl.semaphore_wait(ready.at[3], 1))
    start_peer()
    for i in (1, 0):

        @pl.when(axes[i][0] == 0)
        def _(i=i):
            pl.semaphore_wait(ready.at[i], 1)
            begin(i)

    pl.when(z == 0)(lambda: pl.semaphore_wait(ready.at[2], 1))
    c_ref[...] = jnp.zeros_like(c_ref)

    def forward(t, s):
        known = isinstance(t, int)
        n = t * SUBS + s
        y_wait(n)
        z_start(n)
        if not known or n + AHEAD <= TOTAL:
            y_start(n + AHEAD)
        if s % WIDE == WIDE - 1:
            m = t * B_SUBS + s // WIDE
            x_wait(m)
            d_start(m)
            if not known or m + B_AHEAD < B_TOTAL:
                x_start(m + B_AHEAD)

    def body(t, carry):
        for s in range(SUBS):
            forward(t, s)
            dt, i = (s - LAG) // SUBS - 1, (s - LAG) % SUBS
            if i % 2 == 0:

                @pl.when(t + dt >= 0)
                def _(dt=dt, i=i):
                    if i == 0:
                        pl.when(t + dt == 0)(wait_local)
                        settle(t + dt)
                    product(t + dt, i // 2)

        return carry

    lax.fori_loop(0, TAIL // SUBS, body, 0)

    prior = LAST - 1
    work = {}
    for t in (prior - 2, prior - 1):
        for p in range(SUBS // 2):
            work.setdefault((t + 1) * SUBS + LAG + 2 * p, []).append((t, p, None))
    for p in range(SUBS // 2):
        work.setdefault(FIRST_HALF[p], []).append((prior, p, 0))
        work.setdefault(SECOND_HALF[p], []).append((prior, p, 1))
    for n in range(TAIL, TOTAL):
        forward(n // SUBS, n % SUBS)
        for t, p, half in work.get(n, ()):
            if half is None:
                if p == 0:
                    settle(t)
                product(t, p)
                continue
            if p == 0 and half == 0:
                take(bbuf.at[t, lanes(peer_across)], step_sem(dr, t))
            if p == 0 and half == 1:
                take(abuf.at[t, :, lanes(2 * (1 - y) + 1 - z)], step_sem(zr, t))
            half_product(t, p, (y, 1 - y)[half])
    mine = lanes(2 * (1 - y) + 1 - z)
    early = EARLY * PIECE
    assert early * CHUNK + CHUNK * quarter == (early // 4 + quarter // 4) * 4 * CHUNK
    take(a_last.at[pl.ds(0, early // 4 + quarter // 4)], zr.at[STEP_RING])
    for i in range(EARLY):
        rows = pl.ds(i * PIECE, PIECE)
        c_ref[rows] += jnp.dot(a_last[rows], b_last[...], preferred_element_type=jnp.float32)
    take(a_last.at[pl.ds(early, SUBS * PIECE - early), mine], step_sem(zr, LAST))
    take(a_ref, sent.at[0])
    take(abuf.at[pl.ds(0, 8), pl.ds(0, 1200)], sent.at[1])


def _finish(c_part, a_last, b_last, c_ref, done, sem):
    early = pl.ds(0, EARLY * PIECE)
    pltpu.make_async_copy(c_part.at[early], c_ref.at[early], sem).start()
    for i in range(EARLY, SUBS):
        rows = pl.ds(i * PIECE, PIECE)
        done[rows] = c_part[rows] + jnp.dot(a_last[rows], b_last[...], preferred_element_type=jnp.float32)
        pltpu.make_async_copy(done.at[rows], c_ref.at[rows], sem).start()
    pltpu.make_async_copy(c_part, c_ref, sem).wait()


def solution(mesh):
    def local_product(a_blk, b_blk):
        rows, half = a_blk.shape
        piece = half // 2
        vmem = pl.BlockSpec(memory_space=pltpu.VMEM)
        hbm = pl.BlockSpec(memory_space=pltpu.HBM)
        parts = pl.pallas_call(
            _exchange,
            out_shape=[
                jax.ShapeDtypeStruct((rows, piece), jnp.float32),
                jax.ShapeDtypeStruct((rows, 4 * CHUNK), jnp.bfloat16),
                jax.ShapeDtypeStruct((4 * CHUNK, piece), jnp.bfloat16),
            ],
            in_specs=[hbm, hbm],
            out_specs=[vmem] * 3,
            scratch_shapes=[
                pltpu.VMEM((LAST, rows, 4 * CHUNK), jnp.bfloat16),
                pltpu.VMEM((LAST, 4 * CHUNK, piece), jnp.bfloat16),
                pltpu.SemaphoreType.DMA((RING,)),
                pltpu.SemaphoreType.DMA((STEP_RING + 1,)),
                pltpu.SemaphoreType.DMA((B_RING,)),
                pltpu.SemaphoreType.DMA((STEP_RING + 1,)),
                pltpu.SemaphoreType.DMA((2,)),
                pltpu.SemaphoreType.DMA((2,)),
                pltpu.SemaphoreType.REGULAR((4,)),
            ],
            compiler_params=pltpu.CompilerParams(collective_id=0, has_side_effects=True, vmem_limit_bytes=LIMIT),
        )(a_blk, b_blk)
        return pl.pallas_call(
            _finish,
            out_shape=jax.ShapeDtypeStruct((rows, piece), jnp.float32),
            in_specs=[vmem] * 3,
            out_specs=hbm,
            scratch_shapes=[pltpu.VMEM((rows, piece), jnp.float32), pltpu.SemaphoreType.DMA],
            compiler_params=pltpu.CompilerParams(vmem_limit_bytes=LIMIT_FINISH),
        )(*parts)

    return jax.shard_map(
        local_product,
        mesh=mesh,
        in_specs=(P("row", "col"), P("row", "col")),
        out_specs=P("row", ("col", "dep")),
        check_vma=False,
    )
```

```python
import jax
import jax.numpy as jnp
from jax import lax
from jax.experimental import pallas as pl
from jax.experimental.pallas import tpu as pltpu
from jax.sharding import PartitionSpec as P

MESH = pl.DeviceIdType.MESH
STEPS = 10
SUBS = 10
CHUNK = 128
PIECE = 128
COLS = 256
TOTAL = STEPS * SUBS
LAST = STEPS - 1
EXTRA = 464
EARLY = 2
AHEAD = 7
WIDE = 5
B_AHEAD = 2
FIRST_HALF = (91, 93, 95, 97, 97)
SECOND_HALF = (97, 98, 98, 99, 99)
LAG = 6
RING = 2 * AHEAD
B_RING = 2 * B_AHEAD
B_SUBS = SUBS // WIDE
B_TOTAL = STEPS * B_SUBS
STEP_RING = 3
TAIL = (STEPS - 2) * SUBS
LIMIT = 42 * 2**20
LIMIT_FINISH = 20 * 2**20


def _exchange(a_ref, b_ref, c_ref, a_last, b_last, abuf, bbuf, yr, zr, xr, dr, sent, local, ready):
    z, y, r = lax.axis_index("dep"), lax.axis_index("col"), lax.axis_index("row")
    quarter = a_ref.shape[1] // 2
    across = lax.rem(r + 2, 4)
    peer = r + 1 - 2 * lax.rem(r, 2)
    peer_across = lax.rem(peer + 2, 4)
    to_y, to_z, to_x, to_d = {"col": 1 - y}, {"dep": 1 - z}, {"row": across}, {"row": peer}

    def aligned(start, size):
        return pl.ds(pl.multiple_of(start, CHUNK), size)

    def lanes(q):
        return aligned(q * CHUNK, CHUNK)

    def remote(src, dst, send, recv, to):
        return pltpu.make_async_remote_copy(
            src_ref=src, dst_ref=dst, send_sem=send, recv_sem=recv, device_id=to, device_id_type=MESH
        )

    def is_last(t):
        return isinstance(t, int) and t == LAST

    def a_step(t):
        return a_last if is_last(t) else abuf.at[t]

    def b_step(t):
        return b_last if is_last(t) else bbuf.at[t]

    def a_slot(n, q):
        return a_step(n // SUBS).at[aligned((n % SUBS) * PIECE, PIECE), lanes(q)]

    def b_slot(n, q):
        return b_step(n // B_SUBS).at[lanes(q), aligned((n % B_SUBS) * WIDE * PIECE, WIDE * PIECE)]

    def take(some, sem):
        pltpu.make_async_copy(some, some, sem).wait()

    def step_sem(sems, t):
        return sems.at[lax.rem(t, STEP_RING)]

    def y_start(n):
        if isinstance(n, int) and n == TOTAL:
            rows = pl.ds(SUBS * PIECE - EXTRA, EXTRA)
            src = a_ref.at[rows, aligned((1 - z) * quarter + LAST * CHUNK, CHUNK)]
            remote(src, a_last.at[rows, lanes(2 * y + 1 - z)], sent.at[0], step_sem(zr, LAST), to_y).start()
            return
        src = a_ref.at[aligned((n % SUBS) * PIECE, PIECE), aligned(z * quarter + n // SUBS * CHUNK, CHUNK)]
        remote(src, a_slot(n, 2 * y + z), sent.at[0], yr.at[lax.rem(n, RING)], to_y).start()

    def y_wait(n):
        take(a_slot(n, 2 * (1 - y) + z), yr.at[lax.rem(n, RING)])

    def z_start(n):
        slot, recv = a_slot(n, 2 * (1 - y) + z), step_sem(zr, n // SUBS)
        if is_last(n // SUBS):
            i = n % SUBS
            size = min(PIECE, SUBS * PIECE - EXTRA - i * PIECE)
            if size <= 0:
                return
            slot = a_last.at[pl.ds(i * PIECE, size), lanes(2 * (1 - y) + z)]
            recv = zr.at[STEP_RING] if i < EARLY else recv
        remote(slot, slot, sent.at[0], recv, to_z).start()

    def x_start(n):
        columns = aligned(z * quarter + (n % B_SUBS) * WIDE * PIECE, WIDE * PIECE)
        src = b_ref.at[aligned(n // B_SUBS * CHUNK, CHUNK), columns]
        remote(src, b_slot(n, r), sent.at[1], xr.at[lax.rem(n, B_RING)], to_x).start()

    def x_wait(n):
        take(b_slot(n, across), xr.at[lax.rem(n, B_RING)])

    def d_start(n):
        slot = b_slot(n, across)
        t = n // B_SUBS
        remote(slot, slot, sent.at[1], zr.at[STEP_RING] if is_last(t) else step_sem(dr, t), to_d).start()

    def settle(t):
        take(abuf.at[t, :, lanes(2 * (1 - y) + 1 - z)], step_sem(zr, t))
        take(bbuf.at[t, lanes(peer_across)], step_sem(dr, t))

    def start_local():
        for t in range(STEPS):
            for part in range(2):
                src = a_ref.at[:, pl.ds(part * quarter + t * CHUNK, CHUNK)]
                pltpu.make_async_copy(src, a_step(t).at[:, lanes(2 * y + part)], local.at[0]).start()
            src = b_ref.at[pl.ds(t * CHUNK, CHUNK), aligned(z * quarter, quarter)]
            dst = b_step(t).at[lanes(r)]
            pltpu.make_async_copy(src, dst, local.at[0]).start()

    def start_peer():
        for t in range(STEPS):
            src = b_ref.at[pl.ds(t * CHUNK, CHUNK), aligned(z * quarter, quarter)]
            remote(src, b_step(t).at[lanes(r)], sent.at[1], local.at[1], to_d).start()

    def wait_local():
        take(abuf.at[pl.ds(0, 8), pl.ds(0, 1200)], local.at[0])
        take(b_ref.at[:, pl.ds(0, quarter)], local.at[1])

    def product(t, p):
        cols = pl.ds(p * COLS, COLS)
        c_ref[:, cols] += jnp.dot(abuf[t], bbuf[t, :, cols], preferred_element_type=jnp.float32)

    x, core = r // 2, lax.rem(r, 2)
    axes = ((x, to_x), (y, to_y), (z, to_z), (1 - core, to_d))
    def half_product(t, p, side):
        cols, half = pl.ds(p * COLS, COLS), aligned(side * 2 * CHUNK, 2 * CHUNK)
        c_ref[:, cols] += jnp.dot(abuf[t, :, half], bbuf[t, half, cols], preferred_element_type=jnp.float32)

    barrier = pltpu.get_barrier_semaphore()
    for at, to in axes:

        @pl.when(at == 0)
        def _(to=to):
            pl.semaphore_signal(barrier, inc=1, device_id=to, device_id_type=MESH)

    ahead = x + y + z + 1 - core
    pl.when(ahead > 0)(lambda: pl.semaphore_wait(barrier, ahead))
    for i, (at, to) in enumerate(axes):

        @pl.when(at == 1)
        def _(i=i, to=to):
            pl.semaphore_signal(ready.at[i], inc=1, device_id=to, device_id_type=MESH)

    def begin(i):
        for n in range((B_AHEAD, AHEAD)[i]):
            (x_start, y_start)[i](n)

    pl.when(y == 1)(lambda: begin(1))
    pl.when(x == 1)(lambda: begin(0))
    start_local()
    pl.when(core == 1)(lambda: pl.semaphore_wait(ready.at[3], 1))
    start_peer()
    for i in (1, 0):

        @pl.when(axes[i][0] == 0)
        def _(i=i):
            pl.semaphore_wait(ready.at[i], 1)
            begin(i)

    pl.when(z == 0)(lambda: pl.semaphore_wait(ready.at[2], 1))
    c_ref[...] = jnp.zeros_like(c_ref)

    def forward(t, s):
        known = isinstance(t, int)
        n = t * SUBS + s
        y_wait(n)
        z_start(n)
        if not known or n + AHEAD <= TOTAL:
            y_start(n + AHEAD)
        if s % WIDE == WIDE - 1:
            m = t * B_SUBS + s // WIDE
            x_wait(m)
            d_start(m)
            if not known or m + B_AHEAD < B_TOTAL:
                x_start(m + B_AHEAD)

    def body(t, carry):
        for s in range(SUBS):
            forward(t, s)
            dt, i = (s - LAG) // SUBS - 1, (s - LAG) % SUBS
            if i % 2 == 0:

                @pl.when(t + dt >= 0)
                def _(dt=dt, i=i):
                    if i == 0:
                        pl.when(t + dt == 0)(wait_local)
                        settle(t + dt)
                    product(t + dt, i // 2)

        return carry

    lax.fori_loop(0, TAIL // SUBS, body, 0)

    prior = LAST - 1
    work = {}
    for t in (prior - 2, prior - 1):
        for p in range(SUBS // 2):
            work.setdefault((t + 1) * SUBS + LAG + 2 * p, []).append((t, p, None))
    for p in range(SUBS // 2):
        work.setdefault(FIRST_HALF[p], []).append((prior, p, 0))
        work.setdefault(SECOND_HALF[p], []).append((prior, p, 1))
    for n in range(TAIL, TOTAL):
        forward(n // SUBS, n % SUBS)
        for t, p, half in work.get(n, ()):
            if half is None:
                if p == 0:
                    settle(t)
                product(t, p)
                continue
            if p == 0 and half == 0:
                take(bbuf.at[t, lanes(peer_across)], step_sem(dr, t))
            if p == 0 and half == 1:
                take(abuf.at[t, :, lanes(2 * (1 - y) + 1 - z)], step_sem(zr, t))
            half_product(t, p, (y, 1 - y)[half])
    mine = lanes(2 * (1 - y) + 1 - z)
    early = EARLY * PIECE
    assert early * CHUNK + CHUNK * quarter == (early // 4 + quarter // 4) * 4 * CHUNK
    take(a_last.at[pl.ds(0, early // 4 + quarter // 4)], zr.at[STEP_RING])
    for i in range(EARLY):
        rows = pl.ds(i * PIECE, PIECE)
        c_ref[rows] += jnp.dot(a_last[rows], b_last[...], preferred_element_type=jnp.float32)
    take(a_last.at[pl.ds(early, SUBS * PIECE - early), mine], step_sem(zr, LAST))
    take(a_ref, sent.at[0])
    take(abuf.at[pl.ds(0, 8), pl.ds(0, 1200)], sent.at[1])


def _finish(c_part, a_last, b_last, c_ref, done, sem):
    early = pl.ds(0, EARLY * PIECE)
    pltpu.make_async_copy(c_part.at[early], c_ref.at[early], sem).start()
    for i in range(EARLY, SUBS):
        rows = pl.ds(i * PIECE, PIECE)
        done[rows] = c_part[rows] + jnp.dot(a_last[rows], b_last[...], preferred_element_type=jnp.float32)
        pltpu.make_async_copy(done.at[rows], c_ref.at[rows], sem).start()
    pltpu.make_async_copy(c_part, c_ref, sem).wait()


def solution(mesh):
    def local_product(a_blk, b_blk):
        rows, half = a_blk.shape
        piece = half // 2
        vmem = pl.BlockSpec(memory_space=pltpu.VMEM)
        hbm = pl.BlockSpec(memory_space=pltpu.HBM)
        parts = pl.pallas_call(
            _exchange,
            out_shape=[
                jax.ShapeDtypeStruct((rows, piece), jnp.float32),
                jax.ShapeDtypeStruct((rows, 4 * CHUNK), jnp.bfloat16),
                jax.ShapeDtypeStruct((4 * CHUNK, piece), jnp.bfloat16),
            ],
            in_specs=[hbm, hbm],
            out_specs=[vmem] * 3,
            scratch_shapes=[
                pltpu.VMEM((LAST, rows, 4 * CHUNK), jnp.bfloat16),
                pltpu.VMEM((LAST, 4 * CHUNK, piece), jnp.bfloat16),
                pltpu.SemaphoreType.DMA((RING,)),
                pltpu.SemaphoreType.DMA((STEP_RING + 1,)),
                pltpu.SemaphoreType.DMA((B_RING,)),
                pltpu.SemaphoreType.DMA((STEP_RING + 1,)),
                pltpu.SemaphoreType.DMA((2,)),
                pltpu.SemaphoreType.DMA((2,)),
                pltpu.SemaphoreType.REGULAR((4,)),
            ],
            compiler_params=pltpu.CompilerParams(collective_id=0, has_side_effects=True, vmem_limit_bytes=LIMIT),
        )(a_blk, b_blk)
        return pl.pallas_call(
            _finish,
            out_shape=jax.ShapeDtypeStruct((rows, piece), jnp.float32),
            in_specs=[vmem] * 3,
            out_specs=hbm,
            scratch_shapes=[pltpu.VMEM((rows, piece), jnp.float32), pltpu.SemaphoreType.DMA],
            compiler_params=pltpu.CompilerParams(vmem_limit_bytes=LIMIT_FINISH),
        )(*parts)

    return jax.shard_map(
        local_product,
        mesh=mesh,
        in_specs=(P("row", "col"), P("row", "col")),
        out_specs=P("row", ("col", "dep")),
        check_vma=False,
    )
```
